32 devices in a mesh: dp: 8 (over y, x, core), mp: 4 (over z).
Axes of the slice: x: 2, y: 2, z: 4, core: 2. Of those that a mesh axis runs over, the one named last changes fastest.
Arguments:
- feature_ids: int32 [8, 2048, 8], P('dp'), may hold values from 0 to 4095
- tables: bfloat16 [8, 4096, 128], P('dp'), may hold values from -5 to 5
- table_of_feature: int32 [8], replicated, may hold values from 0 to 7, each once
- cross_down: bfloat16 [2, 1024, 512], P(None, 'mp'), may hold values from -0.1875 to 0.1875
- cross_up: bfloat16 [2, 1024, 512], P(None, 'mp'), may hold values from -0.125 to 0.125
- cross_bias: float32 [2, 1024], P(None, 'mp'), may hold values from -3 to 3
- tower_weight: bfloat16 [1024, 2048], P('dp', 'mp'), may hold values from -0.1875 to 0.1875
- tower_bias: float32 [2048], P('mp'), may hold values from -3 to 3
Outputs:
- hidden: bfloat16 [2048, 2048], P('dp', 'mp')
The draws below stay inside these ranges and needn't reach their ends.
Inputs may be any that keep to these rules, and one draw needn't show every extreme that they name: `feature_ids`: each id indexes a row of its own table. `table_of_feature`: each table serves exactly one feature.
All inputs are finite; a program needn't handle non-finite values.
Results may differ from the reference program's by a relative error of at most 0.015.
Values may be sent and summed in bfloat16 or wider, within the bound.
A program may use at most 64 MiB of HBM per device.

```python
import math
import jax
import jax.numpy as jnp
import numpy as np
from jax import lax

EMBED = 128
RANK = 512
HID = 2048
VOCAB = 4096
HOTS = 8
LAYERS = 2
FEATS = 8
WIDTH = 1024
BATCH = 2048


def touch_ends(result, key, smallest, top_value):
    dims = result.shape
    index_at = [jax.random.randint(jax.random.fold_in(key, axis), (), 0, dims[axis]) for axis in range(len(dims))]
    result = result.at[tuple(index_at)].set(smallest)
    longest = dims.index(max(dims))
    index_at[longest] = (index_at[longest] + 1) % dims[longest]
    return result.at[tuple(index_at)].set(top_value)


def block_scale(stream_key, dims, split, least, largest):
    gain = 1.0
    for position, parts in split:
        draws = jax.random.uniform(jax.random.fold_in(jax.random.fold_in(stream_key, 6), position), (parts,), jnp.float32, least / len(split), largest / len(split))
        gain = gain * jnp.repeat(jnp.exp(draws), dims[position] // parts).reshape((-1,) + (1,) * (len(dims) - 1 - position))
    return gain


def cumulative_ranks(number_of, skew):
    portions = [(1 << 20) // math.isqrt(standing ** skew) + 1 for standing in range(1, number_of + 1)]
    width = 1 + sum(portions) // (1 << 30)
    return np.cumsum(np.array([max(1, weight // width) for weight in portions]))


def ranked(key, extent, count, skew):
    table = cumulative_ranks(count, skew)
    pick = jax.random.randint(jax.random.fold_in(key, 1), extent, 0, int(table[count - 1]))
    rank = jnp.searchsorted(jnp.asarray(table, jnp.int32), pick, side="right")
    return jax.random.permutation(jax.random.fold_in(key, 2), count)[rank].astype(jnp.int32)


def centred(key, extent, deviation, limit, shards=(), held_as=jnp.bfloat16):
    loudness = block_scale(key, extent, shards, -0.22, 0.18) if shards else 1.0
    result = jax.random.normal(key, extent, jnp.float32) * deviation * loudness
    return jnp.minimum(jnp.maximum(result, -limit), limit).astype(held_as)


def setup_inputs(seed: int = 0) -> dict:
    key_list = jax.random.split(jax.random.key(seed), 9)
    return {
        "feature_ids": touch_ends(ranked(key_list[0], (FEATS, BATCH, HOTS), VOCAB, 2), jax.random.fold_in(key_list[0], 3), 0, VOCAB - 1).astype(jnp.int32),
        "tables": centred(key_list[1], (FEATS, VOCAB, EMBED), 0.35, 5.0, ((0, 8),)),
        "table_of_feature": jax.random.permutation(key_list[2], FEATS).astype(jnp.int32),
        "cross_down": centred(key_list[3], (LAYERS, WIDTH, RANK), WIDTH ** -0.5, 0.1875, ((1, 4),)),
        "cross_up": centred(key_list[4], (LAYERS, WIDTH, RANK), (4 * RANK) ** -0.5, 0.125, ((1, 4),)),
        "cross_bias": centred(key_list[5], (LAYERS, WIDTH), 0.5, 3.0, ((1, 4),), jnp.float32),
        "tower_weight": centred(key_list[6], (WIDTH, HID), WIDTH ** -0.5, 0.1875, ((0, 8), (1, 4))),
        "tower_bias": centred(key_list[7], (HID,), 0.5, 3.0, ((0, 4),), jnp.float32),
    }


def pool_table(pair):
    table, id_rows = pair
    summed = jnp.zeros((id_rows.shape[0], table.shape[1]), jnp.float32)
    for hot_index in range(HOTS):
        summed = summed + jnp.take(table, id_rows[:, hot_index], axis=0).astype(jnp.float32)
    return summed.astype(jnp.bfloat16)


def reference(feature_ids, tables, table_of_feature, cross_down, cross_up, cross_bias, tower_weight, tower_bias):
    pooled = lax.map(pool_table, (tables, feature_ids))
    ordered = jnp.take(pooled, table_of_feature, axis=0)
    embedded = jnp.transpose(ordered, (1, 0, 2)).reshape(BATCH, WIDTH)
    embedded_wide = embedded.astype(jnp.float32)
    crossed = embedded
    for layer_index in range(LAYERS):
        projected = jnp.dot(crossed, cross_down[layer_index], preferred_element_type=jnp.float32).astype(jnp.bfloat16)
        lifted = lax.dot_general(projected, cross_up[layer_index], (((1,), (1,)), ((), ())), preferred_element_type=jnp.float32)
        crossed = (embedded_wide * (lifted + cross_bias[layer_index]) + crossed.astype(jnp.float32)).astype(jnp.bfloat16)
    pre_act = jnp.dot(crossed, tower_weight, preferred_element_type=jnp.float32) + tower_bias
    return jax.nn.relu(pre_act).astype(jnp.bfloat16)
```

```python
import functools

import jax
import jax.numpy as jnp
from jax import lax
from jax.experimental import pallas as pl
from jax.experimental.pallas import tpu as pltpu
from jax.sharding import PartitionSpec as P


def plain_body(
    feature_ids,
    tables,
    table_of_feature,
    cross_down,
    cross_up,
    cross_bias,
    tower_weight,
    tower_bias,
):
    groups = lax.axis_size("dp")
    members = lax.axis_size("mp")
    member = lax.axis_index("mp")
    table_count, batch_size, hot_count = feature_ids.shape
    row_count = batch_size // (groups * members)
    shaped = feature_ids[0].reshape(groups, members, row_count, hot_count)
    own_ids = lax.dynamic_index_in_dim(shaped, member, 1, keepdims=False).reshape(
        groups * row_count, hot_count
    )
    summed = jnp.zeros((groups * row_count, tables.shape[2]), jnp.float32)
    for hot_index in range(hot_count):
        summed = summed + jnp.take(tables[0], own_ids[:, hot_index], axis=0).astype(jnp.float32)
    columns = [summed.astype(jnp.bfloat16)]
    pooled = jnp.stack(columns, axis=1)
    regrouped = lax.all_to_all(pooled, "dp", split_axis=0, concat_axis=1, tiled=True)
    ordered = jnp.take(regrouped, table_of_feature, axis=1)
    by_width = lax.all_to_all(ordered, "mp", split_axis=1, concat_axis=0, tiled=True)
    group_rows = by_width.shape[0]
    embedded = by_width.reshape(group_rows, -1)
    embedded_wide = embedded.astype(jnp.float32)
    crossed = embedded
    layer_total = cross_down.shape[0]
    for layer_index in range(layer_total):
        partial_value = jnp.dot(
            crossed, cross_down[layer_index], preferred_element_type=jnp.float32
        )
        projected = lax.psum(partial_value.astype(jnp.bfloat16), "mp")
        lifted = lax.dot_general(
            projected,
            cross_up[layer_index],
            (((1,), (1,)), ((), ())),
            preferred_element_type=jnp.float32,
        )
        crossed = (
            embedded_wide * (lifted + cross_bias[layer_index]) + crossed.astype(jnp.float32)
        ).astype(jnp.bfloat16)
    full_rows = lax.all_gather(crossed, "mp", axis=1, tiled=True)
    pre_act = jnp.dot(
        full_rows,
        lax.all_gather(tower_weight, "dp", axis=0, tiled=True),
        preferred_element_type=jnp.float32,
    )
    return jax.nn.relu(pre_act + tower_bias).astype(jnp.bfloat16)


MESH = pl.DeviceIdType.MESH
KERNEL_BYTES = 24 * 1024 * 1024


def kernel(
    groups,
    members,
    ids,
    order,
    table,
    down,
    up,
    bias,
    tower,
    tower_bias,
    out,
    table_half,
    table_wide,
    sums,
    outbox,
    pooled,
    weights,
    biases,
    tower_all,
    crossed_all,
    local_sem,
    z_send,
    z_recv,
    plane_send,
    plane_recv,
    pair_send,
    pair_recv,
    bias_send,
    bias_recv,
    tower_send,
    tower_recv,
    tower_pair_send,
    tower_pair_recv,
    pool_send,
    pool_recv,
    cross_send,
    cross_recv,
):
    d = lax.axis_index("dp")
    m = lax.axis_index("mp")
    chips = groups // 2
    q = lax.div(d, 2)
    c = lax.rem(d, 2)
    partner = q * 2 + 1 - c
    layers, block, rank = down.shape
    hots = ids.shape[0] // (groups * sums.shape[0])
    rows, embed = sums.shape
    piece = block // groups
    depth = tower.shape[0]
    pieces = 2 * layers
    sends = []

    def wrap(value, size):
        return lax.rem(value + size, size)

    def send(src, dst, send_sem, recv_sem, to_d, to_m):
        copy = pltpu.make_async_remote_copy(
            src_ref=src,
            dst_ref=dst,
            send_sem=send_sem,
            recv_sem=recv_sem,
            device_id=(to_d, to_m),
            device_id_type=MESH,
        )
        copy.start()
        sends.append(copy)

    def arrived(ref, send_sem, recv_sem):
        pltpu.make_async_remote_copy(
            src_ref=ref,
            dst_ref=ref,
            send_sem=send_sem,
            recv_sem=recv_sem,
            device_id=(partner, m),
            device_id_type=MESH,
        ).wait_recv()

    def same_core(j):
        return wrap(q + j, chips) * 2 + c

    def slot(p, member, device):
        start = pl.multiple_of(member * block + device * piece, piece)
        return weights.at[p, pl.ds(start, piece), :]

    def tower_slot(device):
        return tower_all.at[pl.ds(pl.multiple_of(device * depth, depth), depth), :]

    def source(p):
        return (down, up)[p % 2].at[p // 2]

    table_copy = pltpu.make_async_copy(table.at[0], table_half, local_sem.at[0])
    table_copy.start()
    locals_ = []
    for p in range(pieces):
        start = pl.multiple_of(m * block, block)
        copy = pltpu.make_async_copy(
            source(p), weights.at[p, pl.ds(start, block), :], local_sem.at[1 + p]
        )
        copy.start()
        locals_.append(copy)
    tower_copy = pltpu.make_async_copy(tower, tower_slot(d), local_sem.at[1 + pieces])
    tower_copy.start()
    bias_copy = pltpu.make_async_copy(bias, biases.at[m], local_sem.at[2 + pieces])
    bias_copy.start()

    barrier = pltpu.get_barrier_semaphore()
    for k in range(1, members):
        pl.semaphore_signal(barrier, inc=1, device_id=(d, wrap(m + k, members)), device_id_type=MESH)
    for i in range(1, groups):
        pl.semaphore_signal(barrier, inc=1, device_id=(wrap(d + i, groups), m), device_id_type=MESH)
    pl.semaphore_wait(barrier, members - 1 + groups - 1)

    own = pl.ds(pl.multiple_of(d * piece, piece), piece)
    for p in range(pieces):
        for k in range(1, members):
            send(
                source(p).at[own, :],
                slot(p, m, d),
                z_send.at[p, k],
                z_recv.at[p, k],
                d,
                wrap(m + k, members),
            )
    for k in range(1, members):
        send(bias, biases.at[m], bias_send.at[k], bias_recv.at[k], d, wrap(m + k, members))

    def spread(p):
        for k in range(1, members):
            came = wrap(m - k, members)
            arrived(slot(p, came, d), z_send.at[p, k], z_recv.at[p, k])
            for j in range(1, chips):
                send(
                    slot(p, came, d),
                    slot(p, came, d),
                    plane_send.at[p, k, j],
                    plane_recv.at[p, k, j],
                    same_core(j),
                    m,
                )
            send(
                slot(p, came, d),
                slot(p, came, d),
                plane_send.at[p, k, 0],
                plane_recv.at[p, k, 0],
                partner,
                m,
            )

    def relay(p):
        for k in range(1, members):
            came = wrap(m - k, members)
            for j in range(1, chips):
                here = slot(p, came, same_core(-j))
                arrived(here, plane_send.at[p, k, j], plane_recv.at[p, k, j])
                send(here, here, pair_send.at[p, k, j], pair_recv.at[p, k, j], partner, m)

    def complete(p):
        locals_[p].wait()
        for k in range(1, members):
            came = wrap(m - k, members)
            here = slot(p, came, partner)
            arrived(here, plane_send.at[p, k, 0], plane_recv.at[p, k, 0])
            for j in range(1, chips):
                here = slot(p, came, wrap(q - j, chips) * 2 + 1 - c)
                arrived(here, pair_send.at[p, k, j], pair_recv.at[p, k, j])

    table_copy.wait()
    table_wide[...] = table_half[...].astype(jnp.float32)
    step = 16 if rows % 16 == 0 else 8

    def pool(group):
        def some(index, carry):
            base = index * step
            for r in range(step):
                total = None
                for hot in range(hots):
                    at = ids[(hot * groups + group) * rows + base + r]
                    row = table_wide[pl.ds(at, 1), :]
                    total = row if total is None else total + row
                sums[pl.ds(base + r, 1), :] = total
            return carry

        lax.fori_loop(0, rows // step, some, 0)
        return sums[...].astype(jnp.bfloat16)

    turn = 0
    for i in range(1, groups + 1):
        if i < groups:
            group = wrap(d + i, groups)
            outbox[i] = pool(group)
            send(outbox.at[i], pooled.at[d], pool_send.at[i], pool_recv.at[i], group, m)
        else:
            pooled[d] = pool(d)
        while turn < pieces and (i >= groups or (turn + 1) * groups <= i * pieces):
            spread(turn)
            turn += 1
    tower_copy.wait()
    for j in range(1, chips):
        send(tower, tower_slot(d), tower_send.at[j], tower_recv.at[j], same_core(j), m)
    send(tower, tower_slot(d), tower_send.at[0], tower_recv.at[0], partner, m)

    relay(0)
    for i in range(1, groups):
        arrived(pooled.at[wrap(d - i, groups)], pool_send.at[i], pool_recv.at[i])
    embedded = jnp.concatenate([pooled[order[f]] for f in range(groups)], axis=1)
    embedded_wide = embedded.astype(jnp.float32)
    bias_copy.wait()
    for k in range(1, members):
        arrived(biases.at[wrap(m - k, members)], bias_send.at[k], bias_recv.at[k])
    relay(1)
    crossed = embedded
    for layer in range(layers):
        p = 2 * layer
        complete(p)
        projected = jnp.dot(crossed, weights[p], preferred_element_type=jnp.float32)
        projected = projected.astype(jnp.bfloat16)
        complete(p + 1)
        if p + 2 < pieces:
            relay(p + 2)
        lifted = lax.dot_general(
            projected,
            weights[p + 1],
            (((1,), (1,)), ((), ())),
            preferred_element_type=jnp.float32,
        )
        row = jnp.concatenate([biases[k, layer : layer + 1, :] for k in range(members)], axis=1)
        crossed = (embedded_wide * (lifted + row) + crossed.astype(jnp.float32)).astype(
            jnp.bfloat16
        )
        if p + 3 < pieces:
            relay(p + 3)
    crossed_all[m] = crossed
    for k in range(1, members):
        send(
            crossed_all.at[m],
            crossed_all.at[m],
            cross_send.at[k],
            cross_recv.at[k],
            d,
            wrap(m + k, members),
        )
    for j in range(1, chips):
        here = tower_slot(same_core(-j))
        arrived(here, tower_send.at[j], tower_recv.at[j])
        send(here, here, tower_pair_send.at[j], tower_pair_recv.at[j], partner, m)
    arrived(tower_slot(partner), tower_send.at[0], tower_recv.at[0])
    for j in range(1, chips):
        here = tower_slot(wrap(q - j, chips) * 2 + 1 - c)
        arrived(here, tower_pair_send.at[j], tower_pair_recv.at[j])

    def finish(member):
        value = jnp.dot(crossed_all[member], tower_all[...], preferred_element_type=jnp.float32)
        value = jnp.maximum(value + tower_bias[...], 0.0).astype(jnp.bfloat16)
        out[pl.ds(pl.multiple_of(member * rows, rows), rows), :] = value

    finish(m)
    for k in range(1, members):
        came = wrap(m - k, members)
        arrived(crossed_all.at[came], cross_send.at[k], cross_recv.at[k])
        finish(came)
    for copy in sends:
        copy.wait_send()


def fused_body(
    feature_ids,
    tables,
    table_of_feature,
    cross_down,
    cross_up,
    cross_bias,
    tower_weight,
    tower_bias,
):
    groups = lax.axis_size("dp")
    members = lax.axis_size("mp")
    member = lax.axis_index("mp")
    _, batch_size, hot_count = feature_ids.shape
    rows = batch_size // (groups * members)
    _, vocab, embed = tables.shape
    layers, block, rank = cross_down.shape
    depth, units = tower_weight.shape
    width = block * members
    pieces = 2 * layers
    chips = groups // 2
    shaped = feature_ids[0].T.reshape(hot_count, groups, members, rows)
    own_ids = lax.dynamic_index_in_dim(shaped, member, 2, keepdims=False).reshape(-1)
    dma = pltpu.SemaphoreType.DMA
    anywhere = pl.BlockSpec(memory_space=pl.ANY)
    vmem = pl.BlockSpec(memory_space=pltpu.VMEM)
    smem = pl.BlockSpec(memory_space=pltpu.SMEM)
    return pl.pallas_call(
        functools.partial(kernel, groups, members),
        out_shape=jax.ShapeDtypeStruct((rows * members, units), jnp.bfloat16),
        in_specs=[smem, smem, anywhere, anywhere, anywhere, vmem, anywhere, vmem],
        out_specs=vmem,
        scratch_shapes=[
            pltpu.VMEM((vocab, embed), jnp.bfloat16),
            pltpu.VMEM((vocab, embed), jnp.float32),
            pltpu.VMEM((rows, embed), jnp.float32),
            pltpu.VMEM((groups, rows, embed), jnp.bfloat16),
            pltpu.VMEM((groups, rows, embed), jnp.bfloat16),
            pltpu.VMEM((pieces, width, rank), jnp.bfloat16),
            pltpu.VMEM((members, layers, block), jnp.float32),
            pltpu.VMEM((width, units), jnp.bfloat16),
            pltpu.VMEM((members, rows, width), jnp.bfloat16),
            dma((3 + pieces,)),
            dma((pieces, members)),
            dma((pieces, members)),
            dma((pieces, members, chips)),
            dma((pieces, members, chips)),
            dma((pieces, members, chips)),
            dma((pieces, members, chips)),
            dma((members,)),
            dma((members,)),
            dma((chips,)),
            dma((chips,)),
            dma((chips,)),
            dma((chips,)),
            dma((groups,)),
            dma((groups,)),
            dma((members,)),
            dma((members,)),
        ],
        compiler_params=pltpu.CompilerParams(
            collective_id=0, has_side_effects=True, vmem_limit_bytes=48 * 1024 * 1024
        ),
    )(
        own_ids,
        table_of_feature,
        tables,
        cross_down,
        cross_up,
        cross_bias,
        tower_weight,
        tower_bias.reshape(1, -1),
    )


def body(
    feature_ids,
    tables,
    table_of_feature,
    cross_down,
    cross_up,
    cross_bias,
    tower_weight,
    tower_bias,
):
    groups = lax.axis_size("dp")
    members = lax.axis_size("mp")
    held = 2 * members * (cross_down.size + cross_up.size) + 2 * groups * tower_weight.size
    fits = held <= KERNEL_BYTES and groups % 2 == 0 and tables.shape[0] == 1
    chosen = fused_body if fits else plain_body
    return chosen(
        feature_ids,
        tables,
        table_of_feature,
        cross_down,
        cross_up,
        cross_bias,
        tower_weight,
        tower_bias,
    )


def solution(mesh):
    return jax.shard_map(
        body,
        mesh=mesh,
        in_specs=(
            P("dp", None, None),
            P("dp", None, None),
            P(),
            P(None, "mp", None),
            P(None, "mp", None),
            P(None, "mp"),
            P("dp", "mp"),
            P("mp"),
        ),
        out_specs=P("dp", "mp"),
        check_vma=False,
    )
```

```python
import functools

import jax
import jax.numpy as jnp
from jax import lax
from jax.experimental import pallas as pl
from jax.experimental.pallas import tpu as pltpu
from jax.sharding import PartitionSpec as P


def plain_body(
    feature_ids,
    tables,
    table_of_feature,
    cross_down,
    cross_up,
    cross_bias,
    tower_weight,
    tower_bias,
):
    groups = lax.axis_size("dp")
    members = lax.axis_size("mp")
    member = lax.axis_index("mp")
    table_count, batch_size, hot_count = feature_ids.shape
    row_count = batch_size // (groups * members)
    shaped = feature_ids[0].reshape(groups, members, row_count, hot_count)
    own_ids = lax.dynamic_index_in_dim(shaped, member, 1, keepdims=False).reshape(
        groups * row_count, hot_count
    )
    summed = jnp.zeros((groups * row_count, tables.shape[2]), jnp.float32)
    for hot_index in range(hot_count):
        summed = summed + jnp.take(tables[0], own_ids[:, hot_index], axis=0).astype(jnp.float32)
    columns = [summed.astype(jnp.bfloat16)]
    pooled = jnp.stack(columns, axis=1)
    regrouped = lax.all_to_all(pooled, "dp", split_axis=0, concat_axis=1, tiled=True)
    ordered = jnp.take(regrouped, table_of_feature, axis=1)
    by_width = lax.all_to_all(ordered, "mp", split_axis=1, concat_axis=0, tiled=True)
    group_rows = by_width.shape[0]
    embedded = by_width.reshape(group_rows, -1)
    embedded_wide = embedded.astype(jnp.float32)
    crossed = embedded
    layer_total = cross_down.shape[0]
    for layer_index in range(layer_total):
        partial_value = jnp.dot(
            crossed, cross_down[layer_index], preferred_element_type=jnp.float32
        )
        projected = lax.psum(partial_value.astype(jnp.bfloat16), "mp")
        lifted = lax.dot_general(
            projected,
            cross_up[layer_index],
            (((1,), (1,)), ((), ())),
            preferred_element_type=jnp.float32,
        )
        crossed = (
            embedded_wide * (lifted + cross_bias[layer_index]) + crossed.astype(jnp.float32)
        ).astype(jnp.bfloat16)
    full_rows = lax.all_gather(crossed, "mp", axis=1, tiled=True)
    pre_act = jnp.dot(
        full_rows,
        lax.all_gather(tower_weight, "dp", axis=0, tiled=True),
        preferred_element_type=jnp.float32,
    )
    return jax.nn.relu(pre_act + tower_bias).astype(jnp.bfloat16)


MESH = pl.DeviceIdType.MESH
KERNEL_BYTES = 24 * 1024 * 1024
VMEM_BYTES = (64 * 1024 - 352) * 1024
CHIPS = 4


def kernel(
    groups,
    members,
    ids_hbm,
    order_hbm,
    table,
    down,
    up,
    bias,
    tower,
    tower_bias_hbm,
    out,
    ids,
    order,
    table_half,
    table_wide,
    sums,
    outbox,
    pooled,
    embedded,
    crossed,
    weights,
    biases,
    tower_all,
    tower_bias,
    crossed_all,
    local_sem,
    z_send,
    z_recv,
    plane_send,
    plane_recv,
    diag_send,
    diag_recv,
    pair_send,
    pair_recv,
    bias_send,
    bias_recv,
    t_plane_send,
    t_plane_recv,
    t_diag_send,
    t_diag_recv,
    t_pair_send,
    t_pair_recv,
    pool_send,
    pool_recv,
    cross_send,
    cross_recv,
):
    d = lax.axis_index("dp")
    m = lax.axis_index("mp")
    q = lax.div(d, 2)
    c = lax.rem(d, 2)
    partner = q * 2 + 1 - c
    chip_x = q + 1 - 2 * lax.rem(q, 2)
    chip_y = lax.rem(q + 2, CHIPS)
    chip_z = lax.rem(chip_x + 2, CHIPS)
    chips = (chip_x, chip_y, chip_z)
    layers, block, rank = down.shape
    hots = ids.shape[0]
    rows, embed = sums.shape
    piece = block // groups
    depth = tower.shape[0]
    pieces = 2 * layers
    sends = []
    locals_ = []

    def wrap(value, size):
        return lax.rem(value + size, size)

    def load(src, dst):
        copy = pltpu.make_async_copy(src, dst, local_sem.at[len(locals_)])
        copy.start()
        locals_.append(copy)
        return copy

    def send(src, dst, send_sem, recv_sem, to_d, to_m):
        copy = pltpu.make_async_remote_copy(
            src_ref=src,
            dst_ref=dst,
            send_sem=send_sem,
            recv_sem=recv_sem,
            device_id=(to_d, to_m),
            device_id_type=MESH,
        )
        copy.start()
        sends.append(copy)

    def arrived(ref, send_sem, recv_sem):
        pltpu.make_async_remote_copy(
            src_ref=ref,
            dst_ref=ref,
            send_sem=send_sem,
            recv_sem=recv_sem,
            device_id=(partner, m),
            device_id_type=MESH,
        ).wait_recv()

    def came(k):
        return wrap(m - k, members)

    def goes(k):
        return wrap(m + k, members)

    def slot(p, member, device, half=None):
        length = piece if half is None else piece // 2
        start = member * block + device * piece + (0 if half is None else half * length)
        return weights.at[p, pl.ds(pl.multiple_of(start, length), length), :]

    def tower_slot(device, half=None):
        length = depth if half is None else depth // 2
        start = device * depth + (0 if half is None else half * length)
        return tower_all.at[pl.ds(pl.multiple_of(start, length), length), :]

    def source(p):
        return (down, up)[p % 2].at[p // 2]

    barrier = pltpu.get_barrier_semaphore()
    for k in range(1, members):
        pl.semaphore_signal(barrier, inc=1, device_id=(d, goes(k)), device_id_type=MESH)
    for i in range(1, groups):
        pl.semaphore_signal(barrier, inc=1, device_id=(wrap(d + i, groups), m), device_id_type=MESH)

    ids_copy = load(ids_hbm, ids)
    table_copy = load(table.at[0], table_half)
    weight_copies = []
    for p in range(pieces):
        here = pl.ds(pl.multiple_of(m * block, block), block)
        weight_copies.append(load(source(p), weights.at[p, here, :]))
    bias_copy = load(bias, biases.at[m])
    order_copy = load(order_hbm, order)
    tower_copy = load(tower, tower_slot(d))
    tower_bias_copy = load(tower_bias_hbm, tower_bias)

    def spread(p):
        for k in range(1, members):
            here = slot(p, came(k), d)
            arrived(here, z_send.at[p, k], z_recv.at[p, k])
            send(here, here, plane_send.at[p, k, 0], plane_recv.at[p, k, 0], chip_x * 2 + c, m)
            send(here, here, plane_send.at[p, k, 1], plane_recv.at[p, k, 1], chip_y * 2 + c, m)
            send(here, here, plane_send.at[p, k, 2], plane_recv.at[p, k, 2], partner, m)

    def relay(p):
        for k in range(1, members):
            for j in range(2):
                chip = chips[j]
                here = slot(p, came(k), chip * 2 + c)
                arrived(here, plane_send.at[p, k, j], plane_recv.at[p, k, j])
                half = slot(p, came(k), chip * 2 + c, j)
                send(
                    half,
                    half,
                    diag_send.at[p, k, j],
                    diag_recv.at[p, k, j],
                    chips[1 - j] * 2 + c,
                    m,
                )
                send(here, here, pair_send.at[p, k, j], pair_recv.at[p, k, j], partner, m)

    def finish_diag(p, k):
        for j in range(2):
            half = slot(p, came(k), chip_z * 2 + c, j)
            arrived(half, diag_send.at[p, k, j], diag_recv.at[p, k, j])
        here = slot(p, came(k), chip_z * 2 + c)
        send(here, here, pair_send.at[p, k, 2], pair_recv.at[p, k, 2], partner, m)

    def diag(p):
        for k in range(1, members):
            finish_diag(p, k)

    def complete(p, k):
        if k == 0:
            weight_copies[p].wait()
            return
        here = slot(p, came(k), partner)
        arrived(here, plane_send.at[p, k, 2], plane_recv.at[p, k, 2])
        for j in range(3):
            here = slot(p, came(k), chips[j] * 2 + 1 - c)
            arrived(here, pair_send.at[p, k, j], pair_recv.at[p, k, j])

    def tower_spread():
        here = tower_slot(d)
        send(here, here, t_plane_send.at[0], t_plane_recv.at[0], chip_x * 2 + c, m)
        send(here, here, t_plane_send.at[1], t_plane_recv.at[1], chip_y * 2 + c, m)
        send(here, here, t_plane_send.at[2], t_plane_recv.at[2], partner, m)

    def tower_relay():
        for j in range(2):
            here = tower_slot(chips[j] * 2 + c)
            arrived(here, t_plane_send.at[j], t_plane_recv.at[j])
            half = tower_slot(chips[j] * 2 + c, j)
            send(half, half, t_diag_send.at[j], t_diag_recv.at[j], chips[1 - j] * 2 + c, m)
            send(here, here, t_pair_send.at[j], t_pair_recv.at[j], partner, m)

    def tower_diag():
        for j in range(2):
            half = tower_slot(chip_z * 2 + c, j)
            arrived(half, t_diag_send.at[j], t_diag_recv.at[j])
        here = tower_slot(chip_z * 2 + c)
        send(here, here, t_pair_send.at[2], t_pair_recv.at[2], partner, m)

    def tower_complete():
        arrived(tower_slot(partner), t_plane_send.at[2], t_plane_recv.at[2])
        for j in range(3):
            here = tower_slot(chips[j] * 2 + 1 - c)
            arrived(here, t_pair_send.at[j], t_pair_recv.at[j])

    step = 16 if rows % 16 == 0 else 8

    def pool(group):
        first = pl.multiple_of((group * members + m) * rows, rows)

        def some(index, carry):
            base = pl.multiple_of(index * step, step)
            for r in range(step):
                total = None
                for hot in range(hots):
                    at = ids[hot, first + base + r]
                    row = table_wide[pl.ds(at, 1), :]
                    total = row if total is None else total + row
                sums[pl.ds(base + r, 1), :] = total
            return carry

        lax.fori_loop(0, rows // step, some, 0)
        return sums[...].astype(jnp.bfloat16)

    def pool_out(i):
        outbox[i] = pool(wrap(d + i, groups))

    def pool_away(i):
        to = wrap(d + i, groups)
        send(outbox.at[i], pooled.at[d], pool_send.at[i], pool_recv.at[i], to, m)

    table_copy.wait()
    table_wide[...] = table_half[...].astype(jnp.float32)
    ids_copy.wait()
    early = 2
    for i in range(1, early + 1):
        pool_out(i)
    pl.semaphore_wait(barrier, members - 1 + groups - 1)

    for p in range(pieces):
        for k in range(1, members):
            own = pl.ds(pl.multiple_of(d * piece, piece), piece)
            send(
                source(p).at[own, :],
                slot(p, m, d),
                z_send.at[p, k],
                z_recv.at[p, k],
                d,
                goes(k),
            )
        if p == 0:
            for k in range(1, members):
                send(bias, biases.at[m], bias_send.at[k], bias_recv.at[k], d, goes(k))
    for i in range(1, groups):
        if i > early:
            pool_out(i)
        pool_away(i)
    pooled[d] = pool(d)

    spread(0)
    spread(1)
    relay(0)
    order_copy.wait()
    for i in range(1, groups):
        arrived(pooled.at[wrap(d - i, groups)], pool_send.at[i], pool_recv.at[i])
    per_block = block // embed
    for b in range(members):
        features = [pooled[order[b * per_block + f]] for f in range(per_block)]
        embedded[b] = jnp.concatenate(features, axis=1)
    bias_copy.wait()
    for k in range(1, members):
        arrived(biases.at[came(k)], bias_send.at[k], bias_recv.at[k])
    for p in range(2, pieces):
        spread(p)
        relay(p - 1)
        diag(p - 2)
    relay(pieces - 1)
    tower_copy.wait()
    tower_spread()
    diag(pieces - 2)

    def matching(p, b):
        return weights[p, pl.ds(pl.multiple_of(b * block, block), block), :]

    for layer in range(layers):
        p = 2 * layer
        last = layer == layers - 1
        state = embedded if layer == 0 else crossed
        projected = None
        for k in range(members):
            complete(p, k)
            b = came(k)
            term = jnp.dot(state[b], matching(p, b), preferred_element_type=jnp.float32)
            projected = term if projected is None else projected + term
        projected = projected.astype(jnp.bfloat16)
        for k in range(members):
            if last and k + 1 < members:
                finish_diag(p + 1, k + 1)
            complete(p + 1, k)
            b = came(k)
            lifted = lax.dot_general(
                projected,
                matching(p + 1, b),
                (((1,), (1,)), ((), ())),
                preferred_element_type=jnp.float32,
            )
            wide = embedded[b].astype(jnp.float32)
            value = wide * (lifted + biases[b, layer : layer + 1, :]) + state[b].astype(jnp.float32)
            value = value.astype(jnp.bfloat16)
            if not last:
                crossed[b] = value
                continue
            crossed_all[m, b] = value
            for to in range(1, members):
                send(
                    crossed_all.at[m, b],
                    crossed_all.at[m, b],
                    cross_send.at[k, to],
                    cross_recv.at[k, to],
                    d,
                    goes(to),
                )

    tower_relay()
    tower_diag()
    tower_bias_copy.wait()
    tower_complete()

    def finish(member):
        value = None
        for b in range(members):
            part = jnp.dot(
                crossed_all[member, b],
                tower_all[b * block : (b + 1) * block, :],
                preferred_element_type=jnp.float32,
            )
            value = part if value is None else value + part
        value = jnp.maximum(value + tower_bias[...], 0.0).astype(jnp.bfloat16)
        out[pl.ds(pl.multiple_of(member * rows, rows), rows), :] = value

    finish(m)
    for to in sorted(range(1, members), key=lambda k: min(k, members - k)):
        sender = came(to)
        for k in range(members):
            here = crossed_all.at[sender, wrap(sender - k, members)]
            arrived(here, cross_send.at[k, to], cross_recv.at[k, to])
        finish(sender)
    for copy in sends:
        copy.wait_send()


def fused_body(
    feature_ids,
    tables,
    table_of_feature,
    cross_down,
    cross_up,
    cross_bias,
    tower_weight,
    tower_bias,
):
    groups = lax.axis_size("dp")
    members = lax.axis_size("mp")
    _, batch_size, hot_count = feature_ids.shape
    rows = batch_size // (groups * members)
    _, vocab, embed = tables.shape
    layers, block, rank = cross_down.shape
    depth, units = tower_weight.shape
    width = block * members
    pieces = 2 * layers
    dma = pltpu.SemaphoreType.DMA
    anywhere = pl.BlockSpec(memory_space=pl.ANY)
    vmem = pl.BlockSpec(memory_space=pltpu.VMEM)
    return pl.pallas_call(
        functools.partial(kernel, groups, members),
        out_shape=jax.ShapeDtypeStruct((rows * members, units), jnp.bfloat16),
        in_specs=[anywhere] * 8,
        out_specs=vmem,
        scratch_shapes=[
            pltpu.SMEM((hot_count, batch_size), jnp.int32),
            pltpu.SMEM(table_of_feature.shape, jnp.int32),
            pltpu.VMEM((vocab, embed), jnp.bfloat16),
            pltpu.VMEM((vocab, embed), jnp.float32),
            pltpu.VMEM((rows, embed), jnp.float32),
            pltpu.VMEM((groups, rows, embed), jnp.bfloat16),
            pltpu.VMEM((groups, rows, embed), jnp.bfloat16),
            pltpu.VMEM((members, rows, block), jnp.bfloat16),
            pltpu.VMEM((members, rows, block), jnp.bfloat16),
            pltpu.VMEM((pieces, width, rank), jnp.bfloat16),
            pltpu.VMEM((members, layers, block), jnp.float32),
            pltpu.VMEM((width, units), jnp.bfloat16),
            pltpu.VMEM((1, units), jnp.float32),
            pltpu.VMEM((members, members, rows, block), jnp.bfloat16),
            dma((6 + pieces,)),
            dma((pieces, members)),
            dma((pieces, members)),
            dma((pieces, members, 3)),
            dma((pieces, members, 3)),
            dma((pieces, members, 2)),
            dma((pieces, members, 2)),
            dma((pieces, members, 3)),
            dma((pieces, members, 3)),
            dma((members,)),
            dma((members,)),
            dma((3,)),
            dma((3,)),
            dma((2,)),
            dma((2,)),
            dma((3,)),
            dma((3,)),
            dma((groups,)),
            dma((groups,)),
            dma((members, members)),
            dma((members, members)),
        ],
        compiler_params=pltpu.CompilerParams(
            collective_id=0, has_side_effects=True, vmem_limit_bytes=VMEM_BYTES
        ),
    )(
        feature_ids[0].T,
        table_of_feature,
        tables,
        cross_down,
        cross_up,
        cross_bias,
        tower_weight,
        tower_bias.reshape(1, -1),
    )


def body(
    feature_ids,
    tables,
    table_of_feature,
    cross_down,
    cross_up,
    cross_bias,
    tower_weight,
    tower_bias,
):
    groups = lax.axis_size("dp")
    members = lax.axis_size("mp")
    held = 2 * members * (cross_down.size + cross_up.size) + 2 * groups * tower_weight.size
    fits = held <= KERNEL_BYTES and groups == 2 * CHIPS and tables.shape[0] == 1
    chosen = fused_body if fits else plain_body
    return chosen(
        feature_ids,
        tables,
        table_of_feature,
        cross_down,
        cross_up,
        cross_bias,
        tower_weight,
        tower_bias,
    )


def solution(mesh):
    return jax.shard_map(
        body,
        mesh=mesh,
        in_specs=(
            P("dp", None, None),
            P("dp", None, None),
            P(),
            P(None, "mp", None),
            P(None, "mp", None),
            P(None, "mp"),
            P("dp", "mp"),
            P("mp"),
        ),
        out_specs=P("dp", "mp"),
        check_vma=False,
    )
```

```python
import functools

import jax
import jax.numpy as jnp
from jax import lax
from jax.experimental import pallas as pl
from jax.experimental.pallas import tpu as pltpu
from jax.sharding import PartitionSpec as P


def plain_body(
    feature_ids,
    tables,
    table_of_feature,
    cross_down,
    cross_up,
    cross_bias,
    tower_weight,
    tower_bias,
):
    groups = lax.axis_size("dp")
    members = lax.axis_size("mp")
    member = lax.axis_index("mp")
    table_count, batch_size, hot_count = feature_ids.shape
    row_count = batch_size // (groups * members)
    shaped = feature_ids[0].reshape(groups, members, row_count, hot_count)
    own_ids = lax.dynamic_index_in_dim(shaped, member, 1, keepdims=False).reshape(
        groups * row_count, hot_count
    )
    summed = jnp.zeros((groups * row_count, tables.shape[2]), jnp.float32)
    for hot_index in range(hot_count):
        summed = summed + jnp.take(tables[0], own_ids[:, hot_index], axis=0).astype(jnp.float32)
    columns = [summed.astype(jnp.bfloat16)]
    pooled = jnp.stack(columns, axis=1)
    regrouped = lax.all_to_all(pooled, "dp", split_axis=0, concat_axis=1, tiled=True)
    ordered = jnp.take(regrouped, table_of_feature, axis=1)
    by_width = lax.all_to_all(ordered, "mp", split_axis=1, concat_axis=0, tiled=True)
    group_rows = by_width.shape[0]
    embedded = by_width.reshape(group_rows, -1)
    embedded_wide = embedded.astype(jnp.float32)
    crossed = embedded
    layer_total = cross_down.shape[0]
    for layer_index in range(layer_total):
        partial_value = jnp.dot(
            crossed, cross_down[layer_index], preferred_element_type=jnp.float32
        )
        projected = lax.psum(partial_value.astype(jnp.bfloat16), "mp")
        lifted = lax.dot_general(
            projected,
            cross_up[layer_index],
            (((1,), (1,)), ((), ())),
            preferred_element_type=jnp.float32,
        )
        crossed = (
            embedded_wide * (lifted + cross_bias[layer_index]) + crossed.astype(jnp.float32)
        ).astype(jnp.bfloat16)
    full_rows = lax.all_gather(crossed, "mp", axis=1, tiled=True)
    pre_act = jnp.dot(
        full_rows,
        lax.all_gather(tower_weight, "dp", axis=0, tiled=True),
        preferred_element_type=jnp.float32,
    )
    return jax.nn.relu(pre_act + tower_bias).astype(jnp.bfloat16)


MESH = pl.DeviceIdType.MESH
KERNEL_BYTES = 24 * 1024 * 1024
VMEM_BYTES = (64 * 1024 - 352) * 1024
CHIPS = 4


def kernel(
    groups,
    members,
    ids_hbm,
    order_hbm,
    table,
    down,
    up,
    bias,
    tower,
    tower_bias_hbm,
    out,
    ids,
    order,
    table_half,
    table_wide,
    sums,
    outbox,
    pooled,
    embedded,
    crossed,
    weights,
    biases,
    tower_all,
    tower_bias,
    crossed_all,
    local_sem,
    z_send,
    z_recv,
    plane_send,
    plane_recv,
    diag_send,
    diag_recv,
    pair_send,
    pair_recv,
    bias_send,
    bias_recv,
    t_plane_send,
    t_plane_recv,
    t_diag_send,
    t_diag_recv,
    t_pair_send,
    t_pair_recv,
    pool_send,
    pool_recv,
    cross_send,
    cross_recv,
):
    d = lax.axis_index("dp")
    m = lax.axis_index("mp")
    q = lax.div(d, 2)
    c = lax.rem(d, 2)
    partner = q * 2 + 1 - c
    chip_x = q + 1 - 2 * lax.rem(q, 2)
    chip_y = lax.rem(q + 2, CHIPS)
    chip_z = lax.rem(chip_x + 2, CHIPS)
    chips = (chip_x, chip_y, chip_z)
    layers, block, rank = down.shape
    hots = ids.shape[0]
    rows, embed = sums.shape
    piece = block // groups
    depth = tower.shape[0]
    pieces = 2 * layers
    sends = []
    locals_ = []

    def wrap(value, size):
        return lax.rem(value + size, size)

    def load(src, dst):
        copy = pltpu.make_async_copy(src, dst, local_sem.at[len(locals_)])
        copy.start()
        locals_.append(copy)
        return copy

    def send(src, dst, send_sem, recv_sem, to_d, to_m):
        copy = pltpu.make_async_remote_copy(
            src_ref=src,
            dst_ref=dst,
            send_sem=send_sem,
            recv_sem=recv_sem,
            device_id=(to_d, to_m),
            device_id_type=MESH,
        )
        copy.start()
        sends.append(copy)

    def arrived(ref, send_sem, recv_sem):
        pltpu.make_async_remote_copy(
            src_ref=ref,
            dst_ref=ref,
            send_sem=send_sem,
            recv_sem=recv_sem,
            device_id=(partner, m),
            device_id_type=MESH,
        ).wait_recv()

    def came(k):
        return wrap(m - k, members)

    def goes(k):
        return wrap(m + k, members)

    def slot(p, member, device, half=None):
        length = piece if half is None else piece // 2
        start = member * block + device * piece + (0 if half is None else half * length)
        return weights.at[p, pl.ds(pl.multiple_of(start, length), length), :]

    def tower_slot(device, half=None):
        length = depth if half is None else depth // 2
        start = device * depth + (0 if half is None else half * length)
        return tower_all.at[pl.ds(pl.multiple_of(start, length), length), :]

    def source(p):
        return (down, up)[p % 2].at[p // 2]

    barrier = pltpu.get_barrier_semaphore()
    for k in range(1, members):
        pl.semaphore_signal(barrier, inc=1, device_id=(d, goes(k)), device_id_type=MESH)
    for i in range(1, groups):
        pl.semaphore_signal(barrier, inc=1, device_id=(wrap(d + i, groups), m), device_id_type=MESH)

    ids_copy = load(ids_hbm, ids)
    table_copy = load(table.at[0], table_half)
    weight_copies = []
    for p in range(pieces):
        here = pl.ds(pl.multiple_of(m * block, block), block)
        weight_copies.append(load(source(p), weights.at[p, here, :]))
    bias_copy = load(bias, biases.at[m])
    order_copy = load(order_hbm, order)
    tower_copy = load(tower, tower_slot(d))
    tower_bias_copy = load(tower_bias_hbm, tower_bias)

    def spread(p):
        for k in range(1, members):
            here = slot(p, came(k), d)
            arrived(here, z_send.at[p, k], z_recv.at[p, k])
            send(here, here, plane_send.at[p, k, 0], plane_recv.at[p, k, 0], chip_x * 2 + c, m)
            send(here, here, plane_send.at[p, k, 1], plane_recv.at[p, k, 1], chip_y * 2 + c, m)
            send(here, here, plane_send.at[p, k, 2], plane_recv.at[p, k, 2], partner, m)

    def relay(p):
        for k in range(1, members):
            for j in range(2):
                chip = chips[j]
                here = slot(p, came(k), chip * 2 + c)
                arrived(here, plane_send.at[p, k, j], plane_recv.at[p, k, j])
                half = slot(p, came(k), chip * 2 + c, j)
                send(
                    half,
                    half,
                    diag_send.at[p, k, j],
                    diag_recv.at[p, k, j],
                    chips[1 - j] * 2 + c,
                    m,
                )
                send(here, here, pair_send.at[p, k, j], pair_recv.at[p, k, j], partner, m)

    def finish_diag(p, k):
        for j in range(2):
            half = slot(p, came(k), chip_z * 2 + c, j)
            arrived(half, diag_send.at[p, k, j], diag_recv.at[p, k, j])
        here = slot(p, came(k), chip_z * 2 + c)
        send(here, here, pair_send.at[p, k, 2], pair_recv.at[p, k, 2], partner, m)

    def diag(p):
        for k in range(1, members):
            finish_diag(p, k)

    def complete(p, k):
        if k == 0:
            weight_copies[p].wait()
            return
        here = slot(p, came(k), partner)
        arrived(here, plane_send.at[p, k, 2], plane_recv.at[p, k, 2])
        for j in range(3):
            here = slot(p, came(k), chips[j] * 2 + 1 - c)
            arrived(here, pair_send.at[p, k, j], pair_recv.at[p, k, j])

    def tower_spread():
        here = tower_slot(d)
        send(here, here, t_plane_send.at[0], t_plane_recv.at[0], chip_x * 2 + c, m)
        send(here, here, t_plane_send.at[1], t_plane_recv.at[1], chip_y * 2 + c, m)
        send(here, here, t_plane_send.at[2], t_plane_recv.at[2], partner, m)

    def tower_relay():
        for j in range(2):
            here = tower_slot(chips[j] * 2 + c)
            arrived(here, t_plane_send.at[j], t_plane_recv.at[j])
            half = tower_slot(chips[j] * 2 + c, j)
            send(half, half, t_diag_send.at[j], t_diag_recv.at[j], chips[1 - j] * 2 + c, m)
            send(here, here, t_pair_send.at[j], t_pair_recv.at[j], partner, m)

    def tower_diag():
        for j in range(2):
            half = tower_slot(chip_z * 2 + c, j)
            arrived(half, t_diag_send.at[j], t_diag_recv.at[j])
        here = tower_slot(chip_z * 2 + c)
        send(here, here, t_pair_send.at[2], t_pair_recv.at[2], partner, m)

    def tower_complete():
        arrived(tower_slot(partner), t_plane_send.at[2], t_plane_recv.at[2])
        for j in range(3):
            here = tower_slot(chips[j] * 2 + 1 - c)
            arrived(here, t_pair_send.at[j], t_pair_recv.at[j])

    step = 16 if rows % 16 == 0 else 8

    def pool(group):
        first = pl.multiple_of((group * members + m) * rows, rows)

        def some(index, carry):
            base = pl.multiple_of(index * step, step)
            for r in range(step):
                total = None
                for hot in range(hots):
                    at = ids[hot, first + base + r]
                    row = table_wide[pl.ds(at, 1), :]
                    total = row if total is None else total + row
                sums[pl.ds(base + r, 1), :] = total
            return carry

        lax.fori_loop(0, rows // step, some, 0)
        return sums[...].astype(jnp.bfloat16)

    def pool_out(i):
        outbox[i] = pool(wrap(d + i, groups))

    def pool_away(i):
        to = wrap(d + i, groups)
        send(outbox.at[i], pooled.at[d], pool_send.at[i], pool_recv.at[i], to, m)

    table_copy.wait()
    table_wide[...] = table_half[...].astype(jnp.float32)
    ids_copy.wait()
    early = 2
    for i in range(1, early + 1):
        pool_out(i)
    pl.semaphore_wait(barrier, members - 1 + groups - 1)

    for p in range(pieces):
        for k in range(1, members):
            own = pl.ds(pl.multiple_of(d * piece, piece), piece)
            send(
                source(p).at[own, :],
                slot(p, m, d),
                z_send.at[p, k],
                z_recv.at[p, k],
                d,
                goes(k),
            )
        if p == 0:
            for k in range(1, members):
                send(bias, biases.at[m], bias_send.at[k], bias_recv.at[k], d, goes(k))
    for i in range(1, groups):
        if i > early:
            pool_out(i)
        pool_away(i)
    pooled[d] = pool(d)

    spread(0)
    spread(1)
    relay(0)
    order_copy.wait()
    for i in range(1, groups):
        arrived(pooled.at[wrap(d - i, groups)], pool_send.at[i], pool_recv.at[i])
    per_block = block // embed
    for b in range(members):
        features = [pooled[order[b * per_block + f]] for f in range(per_block)]
        embedded[b] = jnp.concatenate(features, axis=1)
    bias_copy.wait()
    for k in range(1, members):
        arrived(biases.at[came(k)], bias_send.at[k], bias_recv.at[k])
    for p in range(2, pieces):
        spread(p)
        relay(p - 1)
        diag(p - 2)
    relay(pieces - 1)
    tower_copy.wait()
    tower_spread()
    diag(pieces - 2)

    def matching(p, b):
        return weights[p, pl.ds(pl.multiple_of(b * block, block), block), :]

    for layer in range(layers):
        p = 2 * layer
        last = layer == layers - 1
        state = embedded if layer == 0 else crossed
        projected = None
        for k in range(members):
            complete(p, k)
            b = came(k)
            term = jnp.dot(state[b], matching(p, b), preferred_element_type=jnp.float32)
            projected = term if projected is None else projected + term
        projected = projected.astype(jnp.bfloat16)
        for k in range(members):
            if last and k + 1 < members:
                finish_diag(p + 1, k + 1)
            complete(p + 1, k)
            b = came(k)
            lifted = lax.dot_general(
                projected,
                matching(p + 1, b),
                (((1,), (1,)), ((), ())),
                preferred_element_type=jnp.float32,
            )
            wide = embedded[b].astype(jnp.float32)
            value = wide * (lifted + biases[b, layer : layer + 1, :]) + state[b].astype(jnp.float32)
            value = value.astype(jnp.bfloat16)
            if not last:
                crossed[b] = value
                continue
            crossed_all[m, b] = value
            for to in range(1, members):
                send(
                    crossed_all.at[m, b],
                    crossed_all.at[m, b],
                    cross_send.at[k, to],
                    cross_recv.at[k, to],
                    d,
                    goes(to),
                )

    tower_relay()
    tower_diag()
    tower_bias_copy.wait()
    tower_complete()

    def finish(member):
        value = None
        for b in range(members):
            part = jnp.dot(
                crossed_all[member, b],
                tower_all[b * block : (b + 1) * block, :],
                preferred_element_type=jnp.float32,
            )
            value = part if value is None else value + part
        value = jnp.maximum(value + tower_bias[...], 0.0).astype(jnp.bfloat16)
        out[pl.ds(pl.multiple_of(member * rows, rows), rows), :] = value

    finish(m)
    for to in sorted(range(1, members), key=lambda k: min(k, members - k)):
        sender = came(to)
        for k in range(members):
            here = crossed_all.at[sender, wrap(sender - k, members)]
            arrived(here, cross_send.at[k, to], cross_recv.at[k, to])
        finish(sender)
    for copy in sends:
        copy.wait_send()


def fused_body(
    feature_ids,
    tables,
    table_of_feature,
    cross_down,
    cross_up,
    cross_bias,
    tower_weight,
    tower_bias,
):
    groups = lax.axis_size("dp")
    members = lax.axis_size("mp")
    _, batch_size, hot_count = feature_ids.shape
    rows = batch_size // (groups * members)
    _, vocab, embed = tables.shape
    layers, block, rank = cross_down.shape
    depth, units = tower_weight.shape
    width = block * members
    pieces = 2 * layers
    dma = pltpu.SemaphoreType.DMA
    anywhere = pl.BlockSpec(memory_space=pl.ANY)
    vmem = pl.BlockSpec(memory_space=pltpu.VMEM)
    return pl.pallas_call(
        functools.partial(kernel, groups, members),
        out_shape=pltpu.VMEM((rows * members, units), jnp.bfloat16),
        in_specs=[anywhere] * 8,
        out_specs=vmem,
        scratch_shapes=[
            pltpu.SMEM((hot_count, batch_size), jnp.int32),
            pltpu.SMEM(table_of_feature.shape, jnp.int32),
            pltpu.VMEM((vocab, embed), jnp.bfloat16),
            pltpu.VMEM((vocab, embed), jnp.float32),
            pltpu.VMEM((rows, embed), jnp.float32),
            pltpu.VMEM((groups, rows, embed), jnp.bfloat16),
            pltpu.VMEM((groups, rows, embed), jnp.bfloat16),
            pltpu.VMEM((members, rows, block), jnp.bfloat16),
            pltpu.VMEM((members, rows, block), jnp.bfloat16),
            pltpu.VMEM((pieces, width, rank), jnp.bfloat16),
            pltpu.VMEM((members, layers, block), jnp.float32),
            pltpu.VMEM((width, units), jnp.bfloat16),
            pltpu.VMEM((1, units), jnp.float32),
            pltpu.VMEM((members, members, rows, block), jnp.bfloat16),
            dma((6 + pieces,)),
            dma((pieces, members)),
            dma((pieces, members)),
            dma((pieces, members, 3)),
            dma((pieces, members, 3)),
            dma((pieces, members, 2)),
            dma((pieces, members, 2)),
            dma((pieces, members, 3)),
            dma((pieces, members, 3)),
            dma((members,)),
            dma((members,)),
            dma((3,)),
            dma((3,)),
            dma((2,)),
            dma((2,)),
            dma((3,)),
            dma((3,)),
            dma((groups,)),
            dma((groups,)),
            dma((members, members)),
            dma((members, members)),
        ],
        compiler_params=pltpu.CompilerParams(
            collective_id=0, has_side_effects=True, vmem_limit_bytes=VMEM_BYTES
        ),
    )(
        feature_ids[0].T,
        table_of_feature,
        tables,
        cross_down,
        cross_up,
        cross_bias,
        tower_weight,
        tower_bias.reshape(1, -1),
    )


def body(
    feature_ids,
    tables,
    table_of_feature,
    cross_down,
    cross_up,
    cross_bias,
    tower_weight,
    tower_bias,
):
    groups = lax.axis_size("dp")
    members = lax.axis_size("mp")
    held = 2 * members * (cross_down.size + cross_up.size) + 2 * groups * tower_weight.size
    fits = held <= KERNEL_BYTES and groups == 2 * CHIPS and tables.shape[0] == 1
    chosen = fused_body if fits else plain_body
    return chosen(
        feature_ids,
        tables,
        table_of_feature,
        cross_down,
        cross_up,
        cross_bias,
        tower_weight,
        tower_bias,
    )


def solution(mesh):
    return jax.shard_map(
        body,
        mesh=mesh,
        in_specs=(
            P("dp", None, None),
            P("dp", None, None),
            P(),
            P(None, "mp", None),
            P(None, "mp", None),
            P(None, "mp"),
            P("dp", "mp"),
            P("mp"),
        ),
        out_specs=P("dp", "mp"),
        check_vma=False,
    )
```
